32 devices in a mesh: row: 8 (over z, core), col: 4 (over y, x).
Axes of the slice: x: 2, y: 2, z: 4, core: 2. Of those that a mesh axis runs over, the one named last changes fastest.
Arguments:
- energy: float32 [4, 2048, 2048], P('col', 'row'), may hold values from 0.5 to 8
- damage_old: float32 [4, 2048, 2048], P('col', 'row'), may hold values from 0 to 0.8
- crack_seeds: int32 [4, 2048, 2048], P('col', 'row'), may hold values 0 or 1
- irreversible: int32 [4, 2048, 2048], P('col', 'row'), may hold values 0 or 1
- line_inverses: float32 [8, 256, 256], replicated, may hold values from -0.6 to 2.8
- z_inverse: float32 [4, 4], replicated, may hold values from -0.8 to 1.9
Outputs:
- damage: float32 [4, 2048, 2048], P('col', 'row')
- update_norms: float32 [2], replicated
The draws below stay inside these ranges and needn't reach their ends.
All inputs are finite; a program needn't handle non-finite values. No bound on the sum of `crack_seeds` or of `irreversible` on one device may be relied on, other than what follows from the above.
Results may differ from the reference program's by a relative error of at most 0.0001.
Values sent between devices are 32-bit elements; how exact they have to be, the bound alone decides.
A program may use at most 128 MiB of HBM per device.

```python
import math
import jax
import jax.numpy as jnp
from jax import lax

L = 2048
BLK = 256
NBLK = 8
NZ = 4
ITERS = 2


def dominant_blocks(key, block_count, extent, low, high, spread):
    key_diag, key_rest = jax.random.split(key)
    diagonal = jax.random.uniform(key_diag, (block_count, extent), jnp.float32, low, high)
    scatter_part = spread * jax.random.truncated_normal(key_rest, -4.0, 4.0, (block_count, extent, extent), jnp.float32)
    return scatter_part + diagonal[:, :, None] * jnp.eye(extent, dtype=jnp.float32)[None]


def draw_line_inverses(key, part):
    return dominant_blocks(jax.random.fold_in(key, 11), NBLK, BLK, 1.0, 2.0, 0.5 / math.sqrt(BLK))


def draw_z_inverse(key, part):
    return dominant_blocks(jax.random.fold_in(key, 23), 1, NZ, 0.5, 1.0, 0.25 / math.sqrt(NZ))[0]


def plant(array, rng, low, top_value):
    index_at = [jax.random.randint(jax.random.fold_in(rng, axis), (), 0, length) for axis, length in enumerate(array.shape)]
    main_axis = array.shape.index(max(array.shape))
    next_to = index_at[:main_axis] + [(index_at[main_axis] + 1) % array.shape[main_axis]] + index_at[main_axis + 1:]
    return array.at[tuple(index_at)].set(low).at[tuple(next_to)].set(top_value)


def levels(rng, dims, pieces, smallest, high):
    loudness = 1.0
    for dim, blocks in pieces:
        steps = jax.random.uniform(jax.random.fold_in(jax.random.fold_in(rng, 6), dim), (blocks,), jnp.float32, smallest / len(pieces), high / len(pieces))
        loudness = loudness * jnp.repeat(jnp.exp(steps), dims[dim] // blocks).reshape((-1,) + (1,) * (len(dims) - 1 - dim))
    return loudness


def setup_inputs(seed: int = 0) -> dict:
    key_list = jax.random.split(jax.random.key(seed), 7)
    return {
        "energy": jnp.clip(jnp.exp(math.log(8.0) - 2.7725887 * jax.random.uniform(key_list[0], (NZ, L, L), jnp.float32) ** levels(key_list[0], (NZ, L, L), ((0, 4), (1, 8)), -0.2, 0.2)), 0.5, 8.0),
        "damage_old": jnp.clip(0.8 * jax.random.uniform(key_list[1], (NZ, L, L), jnp.float32) ** levels(key_list[1], (NZ, L, L), ((0, 4), (1, 8)), -0.2, 0.2), 0.0, 0.8),
        "crack_seeds": plant((jax.random.randint(key_list[2], (NZ, L, L), 0, 32) < 1).astype(jnp.int32), jax.random.fold_in(key_list[2], 1), 0, 1),
        "irreversible": plant((jax.random.randint(key_list[3], (NZ, L, L), 0, 2) < 1).astype(jnp.int32), jax.random.fold_in(key_list[3], 1), 0, 1),
        "line_inverses": draw_line_inverses(jax.random.fold_in(key_list[6], 71), 0),
        "z_inverse": draw_z_inverse(jax.random.fold_in(key_list[6], 71), 0),
    }


KAPPA = 2.0
STEP = 0.02
COUPLE = 0.5
EPSILON = 1e-06

def second_difference(grid_field, along):
    extent = grid_field.shape[along]
    forward_diff = lax.slice_in_dim(grid_field, 1, extent, axis=along) - lax.slice_in_dim(grid_field, 0, extent - 1, axis=along)
    zero_shape = list(grid_field.shape)
    zero_shape[along] = 1
    zero_rim = jnp.zeros(zero_shape, grid_field.dtype)
    ahead = jnp.concatenate([forward_diff, zero_rim], axis=along)
    behind = jnp.concatenate([zero_rim, forward_diff], axis=along)
    return ahead - behind

def line_solve(line_rows, inverses):
    block_count, block_cells, _ = inverses.shape
    line_count = line_rows.shape[0]
    blocks = line_rows.reshape(line_count, block_count, block_cells)
    products = jnp.einsum('rkb,kcb->rkc', blocks, inverses, precision=lax.Precision.HIGHEST)
    first_col = inverses[:, :, 0]
    last_col = inverses[:, :, block_cells - 1]
    incoming = [jnp.zeros((line_count,), line_rows.dtype)]
    for block_index in range(block_count - 1):
        incoming.append(products[:, block_index, block_cells - 1] + COUPLE * incoming[block_index] * inverses[block_index, block_cells - 1, 0])
    inflow = jnp.stack(incoming, axis=1)
    forward = products + COUPLE * inflow[:, :, None] * first_col[None]
    head_terms = [jnp.zeros((line_count,), line_rows.dtype) for block_index in range(block_count)]
    carried = forward[:, block_count - 1, 0]
    for block_index in range(block_count - 2, -1, -1):
        head_terms[block_index] = carried
        carried = forward[:, block_index, 0] + COUPLE * carried * inverses[block_index, 0, block_cells - 1]
    outflow = jnp.stack(head_terms, axis=1)
    solved = forward + COUPLE * outflow[:, :, None] * last_col[None]
    return solved.reshape(line_count, block_count * block_cells)

def reference(energy, damage_old, crack_seeds, irreversible, line_inverses, z_inverse):
    seeded = crack_seeds == 1
    damage = jnp.where(seeded, 1.0, damage_old)
    lower_bound = jnp.where(irreversible == 1, damage_old, 0.0)
    line_length = energy.shape[2]
    update_sizes = []
    for sweep_index in range(ITERS):
        laplace = second_difference(damage, 0) + second_difference(damage, 1) + second_difference(damage, 2)
        residual = energy - (1.0 + energy) * damage + KAPPA * laplace
        along_x = line_solve(residual.reshape(-1, line_length), line_inverses).reshape(residual.shape)
        turned = jnp.swapaxes(along_x, 1, 2)
        along_y = line_solve(turned.reshape(-1, line_length), line_inverses).reshape(turned.shape)
        along_z = jnp.einsum('zk,kxy->zxy', z_inverse, along_y, precision=lax.Precision.HIGHEST)
        update = STEP * jnp.swapaxes(along_z, 1, 2)
        clamped = jnp.minimum(jnp.maximum(damage + update, lower_bound), 1.0)
        renewed = jnp.where(seeded, 1.0, clamped)
        update_sizes.append(jnp.sqrt(jnp.mean((renewed - damage) ** 2) + EPSILON) / STEP)
        damage = renewed
    return (damage, jnp.stack(update_sizes))
```

```python
import jax
import jax.numpy as jnp
from jax import lax
from jax.sharding import PartitionSpec as P

ITERS = 2


KAPPA = 2.0
STEP = 0.02
COUPLE = 0.5
EPSILON = 1e-06
HIGHEST = lax.Precision.HIGHEST


def second_difference(grid_field, along):
    extent = grid_field.shape[along]
    forward_diff = lax.slice_in_dim(grid_field, 1, extent, axis=along) - lax.slice_in_dim(
        grid_field, 0, extent - 1, axis=along
    )
    zero_shape = list(grid_field.shape)
    zero_shape[along] = 1
    zero_rim = jnp.zeros(zero_shape, grid_field.dtype)
    ahead = jnp.concatenate([forward_diff, zero_rim], axis=along)
    behind = jnp.concatenate([zero_rim, forward_diff], axis=along)
    return ahead - behind


def line_solve(line_rows, inverses):
    block_count, block_cells, _ = inverses.shape
    line_count = line_rows.shape[0]
    blocks = line_rows.reshape(line_count, block_count, block_cells)
    products = jnp.einsum("rkb,kcb->rkc", blocks, inverses, precision=lax.Precision.HIGHEST)
    first_col = inverses[:, :, 0]
    last_col = inverses[:, :, block_cells - 1]
    incoming = [jnp.zeros((line_count,), line_rows.dtype)]
    for block_index in range(block_count - 1):
        incoming.append(
            products[:, block_index, block_cells - 1]
            + COUPLE * incoming[block_index] * inverses[block_index, block_cells - 1, 0]
        )
    inflow = jnp.stack(incoming, axis=1)
    forward = products + COUPLE * inflow[:, :, None] * first_col[None]
    head_terms = [jnp.zeros((line_count,), line_rows.dtype) for block_index in range(block_count)]
    carried = forward[:, block_count - 1, 0]
    for block_index in range(block_count - 2, -1, -1):
        head_terms[block_index] = carried
        carried = (
            forward[:, block_index, 0]
            + COUPLE * carried * inverses[block_index, 0, block_cells - 1]
        )
    outflow = jnp.stack(head_terms, axis=1)
    solved = forward + COUPLE * outflow[:, :, None] * last_col[None]
    return solved.reshape(line_count, block_count * block_cells)


def local_turned(energy, damage_old, crack_seeds, irreversible, line_inverses, z_inverse):
    planes, rows_here, line_length = energy.shape
    row_count = lax.axis_size("row")
    col_count = lax.axis_size("col")
    total_planes = planes * col_count
    cell_count = total_planes * rows_here * row_count * line_length
    seeded = crack_seeds == 1
    damage = jnp.where(seeded, 1.0, damage_old)
    lower_bound = jnp.where(irreversible == 1, damage_old, 0.0)
    own_sums = []
    for sweep_index in range(ITERS):
        local_lap = second_difference(damage, 2)
        partial_value = energy - (1.0 + energy) * damage + KAPPA * local_lap
        moved_part, moved_damage = (
            lax.all_to_all(
                lax.all_to_all(
                    jnp.swapaxes(partial_value, 1, 2),
                    "row",
                    split_axis=1,
                    concat_axis=2,
                    tiled=True,
                ),
                "col",
                split_axis=1,
                concat_axis=0,
                tiled=True,
            ),
            lax.all_to_all(
                lax.all_to_all(
                    jnp.swapaxes(damage, 1, 2), "row", split_axis=1, concat_axis=2, tiled=True
                ),
                "col",
                split_axis=1,
                concat_axis=0,
                tiled=True,
            ),
        )
        lap_rest = second_difference(moved_damage, 2) + second_difference(moved_damage, 0)
        turned = moved_part + KAPPA * lap_rest
        turned_shape = turned.shape
        along_y = line_solve(turned.reshape(-1, turned_shape[2]), line_inverses).reshape(
            turned_shape
        )
        along_z = jnp.einsum("zk,kxy->zxy", z_inverse, along_y, precision=lax.Precision.HIGHEST)
        gathered = lax.all_to_all(
            lax.all_to_all(along_z, "row", split_axis=2, concat_axis=1, tiled=True),
            "col",
            split_axis=0,
            concat_axis=1,
            tiled=True,
        )
        piece_cells = gathered.shape[1] // (row_count * col_count)
        reordered = gathered.reshape(planes, col_count, row_count, piece_cells, rows_here)
        restored = jnp.transpose(reordered, (0, 4, 2, 1, 3)).reshape(planes, rows_here, line_length)
        update = STEP * line_solve(restored.reshape(-1, line_length), line_inverses).reshape(
            restored.shape
        )
        clamped = jnp.minimum(jnp.maximum(damage + update, lower_bound), 1.0)
        renewed = jnp.where(seeded, 1.0, clamped)
        own_sum = jnp.sum((renewed - damage) ** 2)
        own_sums.append(own_sum)
        damage = renewed
    global_sums = lax.psum(jnp.stack(own_sums), ("row", "col"))
    update_norms = jnp.sqrt(global_sums / cell_count + EPSILON) / STEP
    return (damage, update_norms)


def carry_matrix(inverses):
    block_count, block_cells, _ = inverses.shape
    last = block_cells - 1
    eye = jnp.eye(2 * block_count, dtype=inverses.dtype).reshape(block_count, 2, -1)
    first_of, last_of = eye[:, 0], eye[:, 1]
    incoming = [jnp.zeros_like(first_of[0])]
    for k in range(block_count - 1):
        incoming.append(last_of[k] + COUPLE * incoming[k] * inverses[k, last, 0])
    heads = [first_of[k] + COUPLE * incoming[k] * inverses[k, 0, 0] for k in range(block_count)]
    outgoing = [None] * block_count
    outgoing[block_count - 1] = jnp.zeros_like(first_of[0])
    carried = heads[block_count - 1]
    for k in range(block_count - 2, -1, -1):
        outgoing[k] = carried
        carried = heads[k] + COUPLE * carried * inverses[k, 0, last]
    return COUPLE * jnp.stack([jnp.stack(incoming), jnp.stack(outgoing)], axis=1)


def shift_pairs(count, by):
    return [(i, i + by) for i in range(count) if 0 <= i + by < count]


def difference(field, before, after, axis):
    size = field.shape[axis]
    body = lax.slice_in_dim(field, 1, size, axis=axis)
    head = lax.slice_in_dim(field, 0, size - 1, axis=axis)
    ahead = jnp.concatenate([body, after], axis=axis) - field
    behind = field - jnp.concatenate([before, head], axis=axis)
    return ahead - behind


def local(energy, damage_old, crack_seeds, irreversible, line_inverses, z_inverse):
    planes, rows_here, line_length = energy.shape
    row_count = lax.axis_size("row")
    col_count = lax.axis_size("col")
    row, col = lax.axis_index("row"), lax.axis_index("col")
    block_count, block_cells, _ = line_inverses.shape
    total_planes = planes * col_count
    cell_count = total_planes * rows_here * row_count * line_length
    y_blocks = rows_here // block_cells
    width = line_length // col_count
    x_blocks = width // block_cells
    last = block_cells - 1

    seeded = crack_seeds == 1
    floor = jnp.where(seeded, 1.0, jnp.where(irreversible == 1, damage_old, 0.0))
    start = jnp.where(seeded, 1.0, damage_old)

    def to_columns(a):
        return lax.all_to_all(a, "col", split_axis=2, concat_axis=0, tiled=True)

    energy, damage, floor = to_columns(energy), to_columns(start), to_columns(floor)

    carries = carry_matrix(line_inverses)
    ends = jnp.stack([line_inverses[:, :, 0], line_inverses[:, :, last]], axis=2)
    spread = jnp.einsum("kct,ktn->kcn", ends, carries, precision=HIGHEST)
    g_x = lax.dynamic_slice_in_dim(line_inverses, col * x_blocks, x_blocks, 0)
    h_x = lax.dynamic_slice_in_dim(spread, col * x_blocks, x_blocks, 0)
    g_y = lax.dynamic_slice_in_dim(line_inverses, row * y_blocks, y_blocks, 0)
    h_y = lax.dynamic_slice_in_dim(spread, row * y_blocks, y_blocks, 0)

    own_sums = []
    for sweep_index in range(ITERS):
        up = lax.ppermute(damage[:, -1:, :], "row", shift_pairs(row_count, 1))
        down = lax.ppermute(damage[:, :1, :], "row", shift_pairs(row_count, -1))
        left = lax.ppermute(damage[:, :, -1], "col", shift_pairs(col_count, 1))[:, :, None]
        right = lax.ppermute(damage[:, :, 0], "col", shift_pairs(col_count, -1))[:, :, None]
        up = jnp.where(row == 0, damage[:, :1, :], up)
        down = jnp.where(row == row_count - 1, damage[:, -1:, :], down)
        left = jnp.where(col == 0, damage[:, :, :1], left)
        right = jnp.where(col == col_count - 1, damage[:, :, -1:], right)
        laplace = (
            difference(damage, left, right, 2)
            + difference(damage, up, down, 1)
            + difference(damage, damage[:1], damage[-1:], 0)
        )
        residual = energy - (1.0 + energy) * damage + KAPPA * laplace
        mixed = jnp.einsum("zk,kyx->zyx", z_inverse, residual, precision=HIGHEST)
        blocks = mixed.reshape(total_planes, y_blocks, block_cells, x_blocks, block_cells)
        products = jnp.einsum("zuakb,kcb->zuakc", blocks, g_x, precision=HIGHEST)
        products = jnp.einsum("zuakc,uda->zudkc", products, g_y, precision=HIGHEST)
        x_ends = jnp.stack([products[..., 0], products[..., last]], axis=4)
        x_ends = lax.all_gather(x_ends, "col", axis=3, tiled=True)
        x_ends = x_ends.reshape(total_planes, y_blocks, block_cells, -1)
        products = products + jnp.einsum("zudn,kcn->zudkc", x_ends, h_x, precision=HIGHEST)
        y_ends = jnp.stack([products[:, :, 0], products[:, :, last]], axis=2)
        y_ends = lax.all_gather(y_ends, "row", axis=1, tiled=True)
        y_ends = y_ends.reshape(total_planes, -1, x_blocks, block_cells)
        solved = products + jnp.einsum("znkc,udn->zudkc", y_ends, h_y, precision=HIGHEST)
        update = STEP * solved.reshape(damage.shape)
        renewed = jnp.minimum(jnp.maximum(damage + update, floor), 1.0)
        own_sums.append(jnp.sum((renewed - damage) ** 2))
        damage = renewed
    damage = lax.all_to_all(damage, "col", split_axis=0, concat_axis=2, tiled=True)
    global_sums = lax.psum(jnp.stack(own_sums), ("row", "col"))
    update_norms = jnp.sqrt(global_sums / cell_count + EPSILON) / STEP
    return (damage, update_norms)


def solution(mesh):
    def local_any(energy, damage_old, crack_seeds, irreversible, line_inverses, z_inverse):
        block_cells = line_inverses.shape[1]
        width = energy.shape[2] // mesh.shape["col"]
        whole_blocks = energy.shape[1] % block_cells == 0 and width % block_cells == 0
        chosen = local if whole_blocks else local_turned
        return chosen(energy, damage_old, crack_seeds, irreversible, line_inverses, z_inverse)

    return jax.shard_map(
        local_any,
        mesh=mesh,
        in_specs=(
            P("col", "row", None),
            P("col", "row", None),
            P("col", "row", None),
            P("col", "row", None),
            P(),
            P(),
        ),
        out_specs=(P("col", "row", None), P()),
        check_vma=False,
    )
```

```python
import functools

import jax
import jax.numpy as jnp
from jax import lax
from jax.experimental import pallas as pl
from jax.experimental.pallas import tpu as pltpu
from jax.sharding import PartitionSpec as P

ITERS = 2


KAPPA = 2.0
STEP = 0.02
COUPLE = 0.5
EPSILON = 1e-06
HIGHEST = lax.Precision.HIGHEST


def second_difference(grid_field, along):
    extent = grid_field.shape[along]
    forward_diff = lax.slice_in_dim(grid_field, 1, extent, axis=along) - lax.slice_in_dim(
        grid_field, 0, extent - 1, axis=along
    )
    zero_shape = list(grid_field.shape)
    zero_shape[along] = 1
    zero_rim = jnp.zeros(zero_shape, grid_field.dtype)
    ahead = jnp.concatenate([forward_diff, zero_rim], axis=along)
    behind = jnp.concatenate([zero_rim, forward_diff], axis=along)
    return ahead - behind


def line_solve(line_rows, inverses):
    block_count, block_cells, _ = inverses.shape
    line_count = line_rows.shape[0]
    blocks = line_rows.reshape(line_count, block_count, block_cells)
    products = jnp.einsum("rkb,kcb->rkc", blocks, inverses, precision=lax.Precision.HIGHEST)
    first_col = inverses[:, :, 0]
    last_col = inverses[:, :, block_cells - 1]
    incoming = [jnp.zeros((line_count,), line_rows.dtype)]
    for block_index in range(block_count - 1):
        incoming.append(
            products[:, block_index, block_cells - 1]
            + COUPLE * incoming[block_index] * inverses[block_index, block_cells - 1, 0]
        )
    inflow = jnp.stack(incoming, axis=1)
    forward = products + COUPLE * inflow[:, :, None] * first_col[None]
    head_terms = [jnp.zeros((line_count,), line_rows.dtype) for block_index in range(block_count)]
    carried = forward[:, block_count - 1, 0]
    for block_index in range(block_count - 2, -1, -1):
        head_terms[block_index] = carried
        carried = (
            forward[:, block_index, 0]
            + COUPLE * carried * inverses[block_index, 0, block_cells - 1]
        )
    outflow = jnp.stack(head_terms, axis=1)
    solved = forward + COUPLE * outflow[:, :, None] * last_col[None]
    return solved.reshape(line_count, block_count * block_cells)


def local_turned(energy, damage_old, crack_seeds, irreversible, line_inverses, z_inverse):
    planes, rows_here, line_length = energy.shape
    row_count = lax.axis_size("row")
    col_count = lax.axis_size("col")
    total_planes = planes * col_count
    cell_count = total_planes * rows_here * row_count * line_length
    seeded = crack_seeds == 1
    damage = jnp.where(seeded, 1.0, damage_old)
    lower_bound = jnp.where(irreversible == 1, damage_old, 0.0)
    own_sums = []
    for sweep_index in range(ITERS):
        local_lap = second_difference(damage, 2)
        partial_value = energy - (1.0 + energy) * damage + KAPPA * local_lap
        moved_part, moved_damage = (
            lax.all_to_all(
                lax.all_to_all(
                    jnp.swapaxes(partial_value, 1, 2),
                    "row",
                    split_axis=1,
                    concat_axis=2,
                    tiled=True,
                ),
                "col",
                split_axis=1,
                concat_axis=0,
                tiled=True,
            ),
            lax.all_to_all(
                lax.all_to_all(
                    jnp.swapaxes(damage, 1, 2), "row", split_axis=1, concat_axis=2, tiled=True
                ),
                "col",
                split_axis=1,
                concat_axis=0,
                tiled=True,
            ),
        )
        lap_rest = second_difference(moved_damage, 2) + second_difference(moved_damage, 0)
        turned = moved_part + KAPPA * lap_rest
        turned_shape = turned.shape
        along_y = line_solve(turned.reshape(-1, turned_shape[2]), line_inverses).reshape(
            turned_shape
        )
        along_z = jnp.einsum("zk,kxy->zxy", z_inverse, along_y, precision=lax.Precision.HIGHEST)
        gathered = lax.all_to_all(
            lax.all_to_all(along_z, "row", split_axis=2, concat_axis=1, tiled=True),
            "col",
            split_axis=0,
            concat_axis=1,
            tiled=True,
        )
        piece_cells = gathered.shape[1] // (row_count * col_count)
        reordered = gathered.reshape(planes, col_count, row_count, piece_cells, rows_here)
        restored = jnp.transpose(reordered, (0, 4, 2, 1, 3)).reshape(planes, rows_here, line_length)
        update = STEP * line_solve(restored.reshape(-1, line_length), line_inverses).reshape(
            restored.shape
        )
        clamped = jnp.minimum(jnp.maximum(damage + update, lower_bound), 1.0)
        renewed = jnp.where(seeded, 1.0, clamped)
        own_sum = jnp.sum((renewed - damage) ** 2)
        own_sums.append(own_sum)
        damage = renewed
    global_sums = lax.psum(jnp.stack(own_sums), ("row", "col"))
    update_norms = jnp.sqrt(global_sums / cell_count + EPSILON) / STEP
    return (damage, update_norms)


def line_kernel(
    shape,
    corners,
    z_inv,
    energy,
    damage_old,
    crack_seeds,
    irreversible,
    inverses,
    out,
    norms,
    start,
    bound,
    ez,
    fz,
    dz,
    mix,
    gx,
    gy,
    gend,
    ab_x,
    ab_y,
    x_send,
    x_all,
    h_send,
    h_recv,
    y_send,
    y_all,
    s_send,
    s_col,
    s_row_send,
    s_row,
    local_sems,
    move_send,
    move_recv,
    back_send,
    back_recv,
    x_ssem,
    x_rsem,
    h_ssem,
    h_rsem,
    v_ssem,
    v_rsem,
    y_ssem,
    y_rsem,
    sc_ssem,
    sc_rsem,
    sr_ssem,
    sr_rsem,
):
    rows, cols, cells, width, x_blocks, blocks, cell_count = shape
    planes = cols
    last = cells - 1
    row, col = lax.axis_index("row"), lax.axis_index("col")
    ends = 8
    tail = 2 * x_blocks - 1

    def slab(who):
        return pl.ds(pl.multiple_of(who * width, width), width)

    def send(src, dst, ssem, rsem, **where):
        copy = pltpu.make_async_remote_copy(
            src_ref=src, dst_ref=dst, send_sem=ssem, recv_sem=rsem,
            device_id=where, device_id_type=pl.DeviceIdType.MESH,
        )
        copy.start()
        return copy

    def dot(a, b, contract):
        return lax.dot_general(
            a, b, (contract, ((), ())), precision=HIGHEST, preferred_element_type=jnp.float32
        )

    fetch = [
        pltpu.make_async_copy(inverses.at[col * x_blocks + j], gx.at[j], local_sems.at[j])
        for j in range(x_blocks)
    ]
    fetch.append(pltpu.make_async_copy(inverses.at[row], gy, local_sems.at[x_blocks]))
    for copy in fetch:
        copy.start()

    moves = []
    inside = pl.ds(8, cells)

    def move(index, src, landing):
        sent = []
        for o in range(1, cols):
            peer = lax.rem(col + o, cols)
            sent.append(
                send(src.at[:, slab(peer)], landing, move_send.at[index, o - 1],
                     move_recv.at[index, o - 1], col=peer)
            )
        moves.append(sent)

    move(0, energy, ez.at[col])

    @pl.loop(0, cells // 16)
    def _(i):
        at = pl.ds(pl.multiple_of(i * 16, 16), 16)
        old = damage_old[at, :]
        seeded = crack_seeds[at, :] == 1
        start[at, :] = jnp.where(seeded, 1.0, old)
        bound[at, :] = jnp.where(seeded, 1.0, jnp.where(irreversible[at, :] == 1, old, 0.0))

    ez[col] = energy[:, slab(col)]
    move(1, start, dz.at[0, col, inside, :])
    dz[0, col, inside, :] = start[:, slab(col)]
    move(2, bound, fz.at[col])
    fz[col] = bound[:, slab(col)]

    lane = lax.broadcasted_iota(jnp.int32, (8, 128), 1)
    sub = lax.broadcasted_iota(jnp.int32, (8, 128), 0)

    def carries(first, own):
        zero = jnp.zeros((8, 128), jnp.float32)
        incoming = [zero]
        for k in range(blocks - 1):
            at_last = jnp.where(lane == first(k) + 1, 1.0, 0.0)
            incoming.append(at_last + COUPLE * corners[1, k] * incoming[k])
        head = [
            jnp.where(lane == first(k), 1.0, 0.0) + COUPLE * corners[0, k] * incoming[k]
            for k in range(blocks)
        ]
        carried = head[blocks - 1]
        outgoing = [zero] * blocks
        for k in range(blocks - 2, -1, -1):
            outgoing[k] = carried
            carried = head[k] + COUPLE * corners[2, k] * carried
        picked = zero
        even = lax.rem(sub, 2) == 0
        for k in range(blocks):
            value = jnp.where(even, incoming[k], outgoing[k])
            picked = picked + jnp.where(own == k, COUPLE * value, 0.0)
        return picked

    half = lax.div(sub, 2)
    ab_x[...] = carries(
        lambda k: ends * (k // x_blocks) + 2 * (k % x_blocks),
        jnp.where(half < x_blocks, col * x_blocks + half, -1),
    )
    ab_y[...] = carries(lambda k: 2 * planes * k + 2 * half, row + 0 * sub)

    for copy in fetch:
        copy.wait()
    pick_row = lax.broadcasted_iota(jnp.int32, (8, cells), 0)
    pick_lane = lax.broadcasted_iota(jnp.int32, (8, cells), 1)
    gend[...] = jnp.zeros_like(gend)
    for j in range(x_blocks):
        pick = ((pick_row == 2 * j) & (pick_lane == 0)) | (
            (pick_row == 2 * j + 1) & (pick_lane == last)
        )
        gend[:, j * cells : (j + 1) * cells] = dot(
            jnp.where(pick, 1.0, 0.0), gx[j], ((1,), (1,))
        )

    wide_row = lax.broadcasted_iota(jnp.int32, (8, width), 0)
    wide_lane = lax.broadcasted_iota(jnp.int32, (8, width), 1)
    edge = lax.div(wide_row, 2) * cells + lax.rem(wide_row, 2) * last
    sel_ends = jnp.where((wide_lane == edge) & (wide_row < 2 * x_blocks), 1.0, 0.0)
    has_left, has_right = col > 0, col < cols - 1
    sel_left = jnp.where((wide_row == tail) & (wide_lane == 0) & has_left, 1.0, 0.0)
    sel_right = jnp.where((wide_row == 0) & (wide_lane == width - 1) & has_right, 1.0, 0.0)
    sel_in = jnp.concatenate([sel_left, sel_right], axis=0)
    degree_x = (
        2.0
        - jnp.where((wide_lane == 0) & jnp.logical_not(has_left), 1.0, 0.0)
        - jnp.where((wide_lane == width - 1) & jnp.logical_not(has_right), 1.0, 0.0)
    )
    at_first, at_last = wide_lane == 0, wide_lane == width - 1
    upper = jnp.where(row > 0, 1.0, 0.0)
    lower = jnp.where(row < rows - 1, 1.0, 0.0)

    def finish(sent):
        for copy in sent:
            copy.wait()

    def line_rows(z):
        return pl.ds(pl.multiple_of(z * cells, cells), cells)

    finish(moves[1])

    totals = []
    for it in range(ITERS):
        @pl.loop(0, planes)
        def _(z):
            h_send[it, :, line_rows(z)] = dot(sel_ends, dz[it, z, inside, :], ((1,), (1,)))

        halo = [
            send(h_send.at[it], h_recv.at[it, pl.ds(0, 8), :], h_ssem.at[it, 0], h_rsem.at[it, 0],
                 col=lax.rem(col + 1, cols)),
            send(h_send.at[it], h_recv.at[it, pl.ds(8, 8), :], h_ssem.at[it, 1], h_rsem.at[it, 1],
                 col=lax.rem(col + cols - 1, cols)),
            send(dz.at[it, :, pl.ds(cells, 8), :], dz.at[it, :, pl.ds(0, 8), :], v_ssem.at[it, 0],
                 v_rsem.at[it, 0], row=lax.rem(row + 1, rows)),
            send(dz.at[it, :, pl.ds(8, 8), :], dz.at[it, :, pl.ds(cells + 8, 8), :],
                 v_ssem.at[it, 1], v_rsem.at[it, 1], row=lax.rem(row + rows - 1, rows)),
        ]
        if it == 0:
            finish(moves[0])
        finish(halo)

        @pl.loop(0, planes)
        def _(z):
            mix[z] = dot(h_recv[it, :, line_rows(z)], sel_in, ((0,), (0,)))

        @pl.loop(0, cells // 8)
        def _(i):
            near = pl.ds(pl.multiple_of(i * 8, 8), 24)
            here = pl.ds(pl.multiple_of(i * 8, 8), 8)
            y_at = wide_row + i * 8
            top = jnp.where(y_at == 0, upper, 1.0)
            bottom = jnp.where(y_at == last, lower, 1.0)
            wins = [dz[it, z, near, :] for z in range(planes)]
            mids = [w[8:16] for w in wins]
            residual = []
            for z in range(planes):
                d = mids[z]
                above = pltpu.roll(wins[z], 1, 0)[8:16]
                below = pltpu.roll(wins[z], 23, 0)[8:16]
                lap = top * (above - d) + bottom * (below - d)
                lap = lap + jnp.where(at_first, 0.0, pltpu.roll(d, 1, 1))
                lap = lap + jnp.where(at_last, 0.0, pltpu.roll(d, width - 1, 1))
                lap = lap + mix[z, here, :] - degree_x * d
                if z > 0:
                    lap = lap + (mids[z - 1] - d)
                if z < planes - 1:
                    lap = lap + (mids[z + 1] - d)
                e = ez[z, here, :]
                residual.append(e - (1.0 + e) * d + KAPPA * lap)
            for z in range(planes):
                total = z_inv[z, 0] * residual[0]
                for k in range(1, planes):
                    total = total + z_inv[z, k] * residual[k]
                mix[z, here, :] = total

        @pl.loop(0, planes)
        def _(z):
            along = jnp.concatenate(
                [
                    dot(mix[z, :, j * cells : (j + 1) * cells], gx[j], ((1,), (1,)))
                    for j in range(x_blocks)
                ],
                axis=1,
            )
            both = dot(gy[...], along, ((1,), (0,)))
            mix[z] = both
            x_send[it, :, line_rows(z)] = dot(sel_ends, both, ((1,), (1,)))

        swaps = []
        for o in range(1, cols):
            swaps.append(
                send(x_send.at[it], x_all.at[it, pl.ds(pl.multiple_of(col * 8, 8), 8), :],
                     x_ssem.at[it, o - 1], x_rsem.at[it, o - 1], col=lax.rem(col + o, cols))
            )
        x_all[it, pl.ds(pl.multiple_of(col * 8, 8), 8), :] = x_send[it]
        finish(swaps)

        for z in range(planes):
            carry = dot(ab_x[:, : cols * 8], x_all[it, :, z * cells : (z + 1) * cells], ((1,), (0,)))
            value = mix[z] + dot(carry, gend[...], ((0,), (0,)))
            mix[z] = value
            y_send[it, 2 * z : 2 * z + 1, :] = value[:1]
            y_send[it, 2 * z + 1 : 2 * z + 2, :] = value[last:]

        swaps = []
        own = pl.ds(pl.multiple_of(row * 2 * planes, 2 * planes), 2 * planes)
        for o in range(1, rows):
            swaps.append(
                send(y_send.at[it], y_all.at[it, own, :], y_ssem.at[it, o - 1],
                     y_rsem.at[it, o - 1], row=lax.rem(row + o, rows))
            )
        y_all[it, own, :] = y_send[it]
        finish(swaps)
        if it == 0:
            finish(moves[2])
        carry_y = dot(ab_y[:, : rows * 2 * planes], y_all[it], ((1,), (0,)))

        squares = jnp.zeros((8, width), jnp.float32)
        for z in range(planes):
            enter, leave = carry_y[2 * z : 2 * z + 1], carry_y[2 * z + 1 : 2 * z + 2]

            def settle(i, acc, z=z, enter=enter, leave=leave):
                here = pl.ds(pl.multiple_of(i * 8, 8), 8)
                padded = pl.ds(pl.multiple_of(i * 8 + 8, 8), 8)
                g_first, g_last = gy[here, 0:1], gy[here, last : last + 1]
                solved = mix[z, here, :] + g_first * enter + g_last * leave
                d = dz[it, z, padded, :]
                renewed = jnp.minimum(jnp.maximum(d + STEP * solved, fz[z, here, :]), 1.0)
                dz[it + 1, z, padded, :] = renewed
                change = renewed - d
                return acc + change * change

            squares = lax.fori_loop(0, cells // 8, settle, squares, unroll=2)
        totals.append(jnp.sum(squares))

    s_send[...] = jnp.where(sub == 0, totals[0], jnp.where(sub == 1, totals[1], 0.0))
    final = dz.at[ITERS]
    shares = []
    for o in range(1, cols):
        shares.append(
            send(s_send, s_col.at[o - 1], sc_ssem.at[o - 1], sc_rsem.at[o - 1],
                 col=lax.rem(col + o, cols))
        )
    backs = []
    for o in range(1, cols):
        peer = lax.rem(col + o, cols)
        backs.append(
            send(final.at[peer, inside, :], out.at[:, slab(col)], back_send.at[o - 1],
                 back_recv.at[o - 1], col=peer)
        )
    out[:, slab(col)] = final[col, inside, :]
    finish(shares)
    total = s_send[...]
    for o in range(1, cols):
        total = total + s_col[o - 1]
    s_row_send[...] = total
    shares = []
    for o in range(1, rows):
        shares.append(
            send(s_row_send, s_row.at[o - 1], sr_ssem.at[o - 1], sr_rsem.at[o - 1],
                 row=lax.rem(row + o, rows))
        )
    finish(shares)
    for o in range(1, rows):
        total = total + s_row[o - 1]
    norms[...] = jnp.sqrt(total / cell_count + EPSILON) / STEP
    finish(backs)


def local(energy, damage_old, crack_seeds, irreversible, line_inverses, z_inverse):
    planes, cells, line_length = energy.shape
    rows, cols = lax.axis_size("row"), lax.axis_size("col")
    blocks, _, _ = line_inverses.shape
    width = line_length // cols
    x_blocks = width // cells
    last = cells - 1
    lines = cols * cells
    shape = (rows, cols, cells, width, x_blocks, blocks, float(cols * rows * cells * line_length))
    corners = jnp.stack(
        [line_inverses[:, 0, 0], line_inverses[:, last, 0], line_inverses[:, 0, last]]
    )
    f32 = jnp.float32
    dma = pltpu.SemaphoreType.DMA
    vmem = pl.BlockSpec(memory_space=pltpu.VMEM)
    smem = pl.BlockSpec(memory_space=pltpu.SMEM)
    damage, norms = pl.pallas_call(
        functools.partial(line_kernel, shape),
        out_shape=(
            jax.ShapeDtypeStruct((cells, line_length), f32),
            jax.ShapeDtypeStruct((8, 128), f32),
        ),
        in_specs=[smem, smem, vmem, vmem, vmem, vmem, pl.BlockSpec(memory_space=pl.ANY)],
        out_specs=(vmem, vmem),
        scratch_shapes=[
            pltpu.VMEM((cells, line_length), f32),
            pltpu.VMEM((cells, line_length), f32),
            pltpu.VMEM((cols, cells, width), f32),
            pltpu.VMEM((cols, cells, width), f32),
            pltpu.VMEM((ITERS + 1, cols, cells + 16, width), f32),
            pltpu.VMEM((cols, cells, width), f32),
            pltpu.VMEM((x_blocks, cells, cells), f32),
            pltpu.VMEM((cells, cells), f32),
            pltpu.VMEM((8, width), f32),
            pltpu.VMEM((8, 128), f32),
            pltpu.VMEM((8, 128), f32),
            pltpu.VMEM((ITERS, 8, lines), f32),
            pltpu.VMEM((ITERS, 8 * cols, lines), f32),
            pltpu.VMEM((ITERS, 8, lines), f32),
            pltpu.VMEM((ITERS, 16, lines), f32),
            pltpu.VMEM((ITERS, 2 * cols, width), f32),
            pltpu.VMEM((ITERS, 2 * cols * rows, width), f32),
            pltpu.VMEM((8, 128), f32),
            pltpu.VMEM((cols - 1, 8, 128), f32),
            pltpu.VMEM((8, 128), f32),
            pltpu.VMEM((rows - 1, 8, 128), f32),
            dma((x_blocks + 1,)),
            dma((3, cols - 1)),
            dma((3, cols - 1)),
            dma((cols - 1,)),
            dma((cols - 1,)),
            dma((ITERS, cols - 1)),
            dma((ITERS, cols - 1)),
            dma((ITERS, 2)),
            dma((ITERS, 2)),
            dma((ITERS, 2)),
            dma((ITERS, 2)),
            dma((ITERS, rows - 1)),
            dma((ITERS, rows - 1)),
            dma((cols - 1,)),
            dma((cols - 1,)),
            dma((rows - 1,)),
            dma((rows - 1,)),
        ],
        compiler_params=pltpu.CompilerParams(
            has_side_effects=True, vmem_limit_bytes=60 * 1024 * 1024
        ),
        name="line_iterations",
    )(
        corners,
        z_inverse,
        energy[0],
        damage_old[0],
        crack_seeds[0],
        irreversible[0],
        line_inverses,
    )
    return damage[None], norms[:ITERS, 0]


def solution(mesh):
    def local_any(energy, damage_old, crack_seeds, irreversible, line_inverses, z_inverse):
        rows, cols = mesh.shape["row"], mesh.shape["col"]
        block_cells = line_inverses.shape[1]
        width = energy.shape[2] // cols
        whole_blocks = (
            energy.shape[0] == 1
            and energy.shape[1] == block_cells
            and width % block_cells == 0
            and 2 * (width // block_cells) <= 8
            and 2 * cols == 8
            and 8 * max(rows, cols) <= 128
            and min(rows, cols) > 2
        )
        chosen = local if whole_blocks else local_turned
        return chosen(energy, damage_old, crack_seeds, irreversible, line_inverses, z_inverse)

    return jax.shard_map(
        local_any,
        mesh=mesh,
        in_specs=(
            P("col", "row", None),
            P("col", "row", None),
            P("col", "row", None),
            P("col", "row", None),
            P(),
            P(),
        ),
        out_specs=(P("col", "row", None), P()),
        check_vma=False,
    )
```

```python
import functools

import jax
import jax.numpy as jnp
from jax import lax
from jax.experimental import pallas as pl
from jax.experimental.pallas import tpu as pltpu
from jax.sharding import PartitionSpec as P

ITERS = 2


KAPPA = 2.0
STEP = 0.02
COUPLE = 0.5
EPSILON = 1e-06
HIGHEST = lax.Precision.HIGHEST


def second_difference(grid_field, along):
    extent = grid_field.shape[along]
    forward_diff = lax.slice_in_dim(grid_field, 1, extent, axis=along) - lax.slice_in_dim(
        grid_field, 0, extent - 1, axis=along
    )
    zero_shape = list(grid_field.shape)
    zero_shape[along] = 1
    zero_rim = jnp.zeros(zero_shape, grid_field.dtype)
    ahead = jnp.concatenate([forward_diff, zero_rim], axis=along)
    behind = jnp.concatenate([zero_rim, forward_diff], axis=along)
    return ahead - behind


def line_solve(line_rows, inverses):
    block_count, block_cells, _ = inverses.shape
    line_count = line_rows.shape[0]
    blocks = line_rows.reshape(line_count, block_count, block_cells)
    products = jnp.einsum("rkb,kcb->rkc", blocks, inverses, precision=lax.Precision.HIGHEST)
    first_col = inverses[:, :, 0]
    last_col = inverses[:, :, block_cells - 1]
    incoming = [jnp.zeros((line_count,), line_rows.dtype)]
    for block_index in range(block_count - 1):
        incoming.append(
            products[:, block_index, block_cells - 1]
            + COUPLE * incoming[block_index] * inverses[block_index, block_cells - 1, 0]
        )
    inflow = jnp.stack(incoming, axis=1)
    forward = products + COUPLE * inflow[:, :, None] * first_col[None]
    head_terms = [jnp.zeros((line_count,), line_rows.dtype) for block_index in range(block_count)]
    carried = forward[:, block_count - 1, 0]
    for block_index in range(block_count - 2, -1, -1):
        head_terms[block_index] = carried
        carried = (
            forward[:, block_index, 0]
            + COUPLE * carried * inverses[block_index, 0, block_cells - 1]
        )
    outflow = jnp.stack(head_terms, axis=1)
    solved = forward + COUPLE * outflow[:, :, None] * last_col[None]
    return solved.reshape(line_count, block_count * block_cells)


def local_turned(energy, damage_old, crack_seeds, irreversible, line_inverses, z_inverse):
    planes, rows_here, line_length = energy.shape
    row_count = lax.axis_size("row")
    col_count = lax.axis_size("col")
    total_planes = planes * col_count
    cell_count = total_planes * rows_here * row_count * line_length
    seeded = crack_seeds == 1
    damage = jnp.where(seeded, 1.0, damage_old)
    lower_bound = jnp.where(irreversible == 1, damage_old, 0.0)
    own_sums = []
    for sweep_index in range(ITERS):
        local_lap = second_difference(damage, 2)
        partial_value = energy - (1.0 + energy) * damage + KAPPA * local_lap
        moved_part, moved_damage = (
            lax.all_to_all(
                lax.all_to_all(
                    jnp.swapaxes(partial_value, 1, 2),
                    "row",
                    split_axis=1,
                    concat_axis=2,
                    tiled=True,
                ),
                "col",
                split_axis=1,
                concat_axis=0,
                tiled=True,
            ),
            lax.all_to_all(
                lax.all_to_all(
                    jnp.swapaxes(damage, 1, 2), "row", split_axis=1, concat_axis=2, tiled=True
                ),
                "col",
                split_axis=1,
                concat_axis=0,
                tiled=True,
            ),
        )
        lap_rest = second_difference(moved_damage, 2) + second_difference(moved_damage, 0)
        turned = moved_part + KAPPA * lap_rest
        turned_shape = turned.shape
        along_y = line_solve(turned.reshape(-1, turned_shape[2]), line_inverses).reshape(
            turned_shape
        )
        along_z = jnp.einsum("zk,kxy->zxy", z_inverse, along_y, precision=lax.Precision.HIGHEST)
        gathered = lax.all_to_all(
            lax.all_to_all(along_z, "row", split_axis=2, concat_axis=1, tiled=True),
            "col",
            split_axis=0,
            concat_axis=1,
            tiled=True,
        )
        piece_cells = gathered.shape[1] // (row_count * col_count)
        reordered = gathered.reshape(planes, col_count, row_count, piece_cells, rows_here)
        restored = jnp.transpose(reordered, (0, 4, 2, 1, 3)).reshape(planes, rows_here, line_length)
        update = STEP * line_solve(restored.reshape(-1, line_length), line_inverses).reshape(
            restored.shape
        )
        clamped = jnp.minimum(jnp.maximum(damage + update, lower_bound), 1.0)
        renewed = jnp.where(seeded, 1.0, clamped)
        own_sum = jnp.sum((renewed - damage) ** 2)
        own_sums.append(own_sum)
        damage = renewed
    global_sums = lax.psum(jnp.stack(own_sums), ("row", "col"))
    update_norms = jnp.sqrt(global_sums / cell_count + EPSILON) / STEP
    return (damage, update_norms)


def line_kernel(
    shape,
    corners,
    z_inv,
    energy,
    damage_hbm,
    seeds_hbm,
    irreversible_hbm,
    inverses,
    out,
    norms,
    damage_old,
    crack_seeds,
    irreversible,
    start,
    bound,
    ez,
    fz,
    dz,
    mix,
    gx,
    gy,
    gx_high,
    gx_low,
    gy_high,
    gy_low,
    h_in,
    gend,
    ab_x,
    ab_y,
    x_send,
    x_all,
    h_send,
    h_recv,
    y_send,
    y_all,
    s_send,
    s_col,
    s_row_send,
    s_row,
    local_sems,
    move_send,
    move_recv,
    back_send,
    back_recv,
    x_ssem,
    x_rsem,
    h_ssem,
    h_rsem,
    v_ssem,
    v_rsem,
    y_ssem,
    y_rsem,
    sc_ssem,
    sc_rsem,
    sr_ssem,
    sr_rsem,
):
    rows, cols, cells, width, x_blocks, blocks, cell_count = shape
    planes = cols
    last = cells - 1
    row, col = lax.axis_index("row"), lax.axis_index("col")
    ends = 8
    tail = 8 - x_blocks

    def slab(who):
        return pl.ds(pl.multiple_of(who * width, width), width)

    def send(src, dst, ssem, rsem, **where):
        copy = pltpu.make_async_remote_copy(
            src_ref=src, dst_ref=dst, send_sem=ssem, recv_sem=rsem,
            device_id=where, device_id_type=pl.DeviceIdType.MESH,
        )
        copy.start()
        return copy

    def dot(a, b, contract):
        return lax.dot_general(
            a, b, (contract, ((), ())), precision=HIGHEST, preferred_element_type=jnp.float32
        )

    def split(a):
        high = a.astype(jnp.bfloat16)
        return high, (a - high.astype(jnp.float32)).astype(jnp.bfloat16)

    def dot3(a, b):
        def part(u, v):
            return jnp.dot(u, v, preferred_element_type=jnp.float32)

        return part(a[0], b[0]) + (part(a[0], b[1]) + part(a[1], b[0]))

    def line_ends(field):
        tile_lane = lax.broadcasted_iota(jnp.int32, (cells, 128), 1)
        packed = field[:, :128]
        for j in range(x_blocks):
            head = field[:, j * cells : j * cells + 128]
            end = field[:, (j + 1) * cells - 128 : (j + 1) * cells]
            if j > 0:
                head = pltpu.roll(head, j, 1)
                end = pltpu.roll(end, 128 - j, 1)
            packed = jnp.where(tile_lane == j, head, packed)
            packed = jnp.where(tile_lane == 127 - j, end, packed)
        turned = packed.T
        at = lax.broadcasted_iota(jnp.int32, (8, cells), 0)
        kept = (at < x_blocks) | (at >= 8 - x_blocks)
        return jnp.where(kept, jnp.where(at < x_blocks, turned[:8], turned[120:]), 0.0)

    fetch = [
        pltpu.make_async_copy(inverses.at[col * x_blocks + j], gx.at[j], local_sems.at[j])
        for j in range(x_blocks)
    ]
    fetch.append(pltpu.make_async_copy(inverses.at[row], gy, local_sems.at[x_blocks]))
    pulls = [
        pltpu.make_async_copy(damage_hbm, damage_old, local_sems.at[x_blocks + 1]),
        pltpu.make_async_copy(seeds_hbm, crack_seeds, local_sems.at[x_blocks + 2]),
        pltpu.make_async_copy(irreversible_hbm, irreversible, local_sems.at[x_blocks + 3]),
        pltpu.make_async_copy(energy.at[:, slab(col)], ez.at[col], local_sems.at[x_blocks + 4]),
    ]

    moves = []
    inside = pl.ds(8, cells)

    def move(index, src, landing, part=slice(None)):
        sent = []
        for o in range(1, cols):
            peer = lax.rem(col + o, cols)
            sent.append(
                send(src.at[part, slab(peer)], landing, move_send.at[index, o - 1],
                     move_recv.at[index, o - 1], col=peer)
            )
        moves.append(sent)

    move(0, energy, ez.at[col])
    for copy in pulls + fetch:
        copy.start()
    for copy in pulls:
        copy.wait()

    @pl.loop(0, cells // 16)
    def _(i):
        at = pl.ds(pl.multiple_of(i * 16, 16), 16)
        old = damage_old[at, :]
        seeded = crack_seeds[at, :] == 1
        start[at, :] = jnp.where(seeded, 1.0, old)
        bound[at, :] = jnp.where(seeded, 1.0, jnp.where(irreversible[at, :] == 1, old, 0.0))

    move(1, start, dz.at[0, col, inside, :])
    dz[0, col, inside, :] = start[:, slab(col)]
    fz[col] = bound[:, slab(col)]

    lane = lax.broadcasted_iota(jnp.int32, (8, 128), 1)
    sub = lax.broadcasted_iota(jnp.int32, (8, 128), 0)

    def carries(first, final, own):
        zero = jnp.zeros((8, 128), jnp.float32)
        incoming = [zero]
        for k in range(blocks - 1):
            at_last = jnp.where(lane == final(k), 1.0, 0.0)
            incoming.append(at_last + COUPLE * corners[1, k] * incoming[k])
        head = [
            jnp.where(lane == first(k), 1.0, 0.0) + COUPLE * corners[0, k] * incoming[k]
            for k in range(blocks)
        ]
        carried = head[blocks - 1]
        outgoing = [zero] * blocks
        for k in range(blocks - 2, -1, -1):
            outgoing[k] = carried
            carried = head[k] + COUPLE * corners[2, k] * carried
        picked = zero
        even = lax.rem(sub, 2) == 0
        for k in range(blocks):
            value = jnp.where(even, incoming[k], outgoing[k])
            picked = picked + jnp.where(own == k, COUPLE * value, 0.0)
        return picked

    half = lax.div(sub, 2)
    ab_x[...] = carries(
        lambda k: ends * (k // x_blocks) + k % x_blocks,
        lambda k: ends * (k // x_blocks) + 7 - k % x_blocks,
        jnp.where(half < x_blocks, col * x_blocks + half, -1),
    )
    ab_y[...] = carries(
        lambda k: 2 * planes * k + 2 * half,
        lambda k: 2 * planes * k + 2 * half + 1,
        row + 0 * sub,
    )

    for copy in fetch:
        copy.wait()
    gend[...] = jnp.zeros_like(gend)
    for j in range(x_blocks):
        turned = gx[j].T
        gx_high[j], gx_low[j] = split(turned)
        block = slice(j * cells, (j + 1) * cells)
        gend[2 * j : 2 * j + 1, block] = turned[:1]
        gend[2 * j + 1 : 2 * j + 2, block] = turned[last:]
    gy_high[...], gy_low[...] = split(gy[...])

    wide_row = lax.broadcasted_iota(jnp.int32, (8, width), 0)
    wide_lane = lax.broadcasted_iota(jnp.int32, (8, width), 1)
    has_left, has_right = col > 0, col < cols - 1
    degree_x = (
        2.0
        - jnp.where((wide_lane == 0) & jnp.logical_not(has_left), 1.0, 0.0)
        - jnp.where((wide_lane == width - 1) & jnp.logical_not(has_right), 1.0, 0.0)
    )
    at_first, at_last = wide_lane == 0, wide_lane == width - 1
    upper = jnp.where(row > 0, 1.0, 0.0)
    lower = jnp.where(row < rows - 1, 1.0, 0.0)

    def finish(sent):
        for copy in sent:
            copy.wait()

    def line_rows(z):
        return pl.ds(pl.multiple_of(z * cells, cells), cells)

    finish(moves[1])

    totals = []
    for it in range(ITERS):
        @pl.loop(0, planes)
        def _(z):
            h_send[it, :, line_rows(z)] = line_ends(dz[it, z, inside, :])

        halo = [
            send(h_send.at[it], h_recv.at[it, pl.ds(0, 8), :], h_ssem.at[it, 0], h_rsem.at[it, 0],
                 col=lax.rem(col + 1, cols)),
            send(h_send.at[it], h_recv.at[it, pl.ds(8, 8), :], h_ssem.at[it, 1], h_rsem.at[it, 1],
                 col=lax.rem(col + cols - 1, cols)),
            send(dz.at[it, :, pl.ds(cells, 8), :], dz.at[it, :, pl.ds(0, 8), :], v_ssem.at[it, 0],
                 v_rsem.at[it, 0], row=lax.rem(row + 1, rows)),
            send(dz.at[it, :, pl.ds(8, 8), :], dz.at[it, :, pl.ds(cells + 8, 8), :],
                 v_ssem.at[it, 1], v_rsem.at[it, 1], row=lax.rem(row + rows - 1, rows)),
        ]
        if it == 0:
            finish(moves[0])
            pieces = [slice(0, cells // 2), slice(cells // 2, cells)]
            move(2, bound, fz.at[col, pieces[0], :], pieces[0])
        finish(halo)

        @pl.loop(0, planes)
        def _(z):
            left = h_recv[it, tail : tail + 1, line_rows(z)]
            right = h_recv[it, 8:9, line_rows(z)]
            at = lax.broadcasted_iota(jnp.int32, (128, cells), 0)
            left = jnp.where((at == 0) & has_left, left, 0.0)
            right = jnp.where((at == 127) & has_right, right, 0.0)
            h_in[z] = (left + right).T

        @pl.loop(0, cells // 8)
        def _(i):
            near = pl.ds(pl.multiple_of(i * 8, 8), 24)
            here = pl.ds(pl.multiple_of(i * 8, 8), 8)
            y_at = wide_row + i * 8
            top = jnp.where(y_at == 0, upper, 1.0)
            bottom = jnp.where(y_at == last, lower, 1.0)
            wins = [dz[it, z, near, :] for z in range(planes)]
            mids = [w[8:16] for w in wins]
            residual = []
            for z in range(planes):
                d = mids[z]
                above = pltpu.roll(wins[z], 1, 0)[8:16]
                below = pltpu.roll(wins[z], 23, 0)[8:16]
                lap = top * (above - d) + bottom * (below - d)
                lap = lap + jnp.where(at_first, 0.0, pltpu.roll(d, 1, 1))
                lap = lap + jnp.where(at_last, 0.0, pltpu.roll(d, width - 1, 1))
                edges = h_in[z, here, :]
                lap = lap + jnp.where(at_first, jnp.tile(edges, (1, width // 128)), 0.0)
                lap = lap + jnp.where(at_last, jnp.tile(edges, (1, width // 128)), 0.0)
                lap = lap - degree_x * d
                if z > 0:
                    lap = lap + (mids[z - 1] - d)
                if z < planes - 1:
                    lap = lap + (mids[z + 1] - d)
                e = ez[z, here, :]
                residual.append(e - (1.0 + e) * d + KAPPA * lap)
            for z in range(planes):
                total = z_inv[z, 0] * residual[0]
                for k in range(1, planes):
                    total = total + z_inv[z, k] * residual[k]
                mix[z, here, :] = total

        @pl.loop(0, planes)
        def _(z):
            along = jnp.concatenate(
                [
                    dot3(
                        split(mix[z, :, j * cells : (j + 1) * cells]), (gx_high[j], gx_low[j])
                    )
                    for j in range(x_blocks)
                ],
                axis=1,
            )
            both = dot3((gy_high[...], gy_low[...]), split(along))
            mix[z] = both
            x_send[it, :, line_rows(z)] = line_ends(both)

        swaps = []
        for o in range(1, cols):
            swaps.append(
                send(x_send.at[it], x_all.at[it, pl.ds(pl.multiple_of(col * 8, 8), 8), :],
                     x_ssem.at[it, o - 1], x_rsem.at[it, o - 1], col=lax.rem(col + o, cols))
            )
        x_all[it, pl.ds(pl.multiple_of(col * 8, 8), 8), :] = x_send[it]
        if it == 0:
            move(3, bound, fz.at[col, pieces[1], :], pieces[1])
        finish(swaps)

        for z in range(planes):
            carry = dot(ab_x[:, : cols * 8], x_all[it, :, z * cells : (z + 1) * cells], ((1,), (0,)))
            value = mix[z] + dot(carry, gend[...], ((0,), (0,)))
            mix[z] = value
            y_send[it, 2 * z : 2 * z + 1, :] = value[:1]
            y_send[it, 2 * z + 1 : 2 * z + 2, :] = value[last:]

        swaps = []
        own = pl.ds(pl.multiple_of(row * 2 * planes, 2 * planes), 2 * planes)
        for o in range(1, rows):
            swaps.append(
                send(y_send.at[it], y_all.at[it, own, :], y_ssem.at[it, o - 1],
                     y_rsem.at[it, o - 1], row=lax.rem(row + o, rows))
            )
        y_all[it, own, :] = y_send[it]
        finish(swaps)
        if it == 0:
            finish(moves[2] + moves[3])
        carry_y = dot(ab_y[:, : rows * 2 * planes], y_all[it], ((1,), (0,)))

        squares = jnp.zeros((8, width), jnp.float32)
        for z in range(planes):
            enter, leave = carry_y[2 * z : 2 * z + 1], carry_y[2 * z + 1 : 2 * z + 2]

            def settle(i, acc, z=z, enter=enter, leave=leave):
                here = pl.ds(pl.multiple_of(i * 8, 8), 8)
                padded = pl.ds(pl.multiple_of(i * 8 + 8, 8), 8)
                g_first, g_last = gy[here, 0:1], gy[here, last : last + 1]
                solved = mix[z, here, :] + g_first * enter + g_last * leave
                d = dz[it, z, padded, :]
                renewed = jnp.minimum(jnp.maximum(d + STEP * solved, fz[z, here, :]), 1.0)
                dz[it + 1, z, padded, :] = renewed
                change = renewed - d
                return acc + change * change

            squares = lax.fori_loop(0, cells // 8, settle, squares, unroll=2)
        totals.append(jnp.sum(squares))

    s_send[...] = jnp.where(sub == 0, totals[0], jnp.where(sub == 1, totals[1], 0.0))
    final = dz.at[ITERS]
    shares = []
    for o in range(1, cols):
        shares.append(
            send(s_send, s_col.at[o - 1], sc_ssem.at[o - 1], sc_rsem.at[o - 1],
                 col=lax.rem(col + o, cols))
        )
    backs = []
    for o in range(1, cols):
        peer = lax.rem(col + o, cols)
        backs.append(
            send(final.at[peer, inside, :], out.at[:, slab(col)], back_send.at[o - 1],
                 back_recv.at[o - 1], col=peer)
        )
    out[:, slab(col)] = final[col, inside, :]
    finish(shares)
    total = s_send[...]
    for o in range(1, cols):
        total = total + s_col[o - 1]
    s_row_send[...] = total
    shares = []
    for o in range(1, rows):
        shares.append(
            send(s_row_send, s_row.at[o - 1], sr_ssem.at[o - 1], sr_rsem.at[o - 1],
                 row=lax.rem(row + o, rows))
        )
    finish(shares)
    for o in range(1, rows):
        total = total + s_row[o - 1]
    norms[...] = jnp.sqrt(total / cell_count + EPSILON) / STEP
    finish(backs)


def local(energy, damage_old, crack_seeds, irreversible, line_inverses, z_inverse):
    planes, cells, line_length = energy.shape
    rows, cols = lax.axis_size("row"), lax.axis_size("col")
    blocks, _, _ = line_inverses.shape
    width = line_length // cols
    x_blocks = width // cells
    last = cells - 1
    lines = cols * cells
    shape = (rows, cols, cells, width, x_blocks, blocks, float(cols * rows * cells * line_length))
    corners = jnp.stack(
        [line_inverses[:, 0, 0], line_inverses[:, last, 0], line_inverses[:, 0, last]]
    )
    f32 = jnp.float32
    dma = pltpu.SemaphoreType.DMA
    vmem = pl.BlockSpec(memory_space=pltpu.VMEM)
    smem = pl.BlockSpec(memory_space=pltpu.SMEM)
    damage, norms = pl.pallas_call(
        functools.partial(line_kernel, shape),
        out_shape=(
            jax.ShapeDtypeStruct((cells, line_length), f32),
            jax.ShapeDtypeStruct((8, 128), f32),
        ),
        in_specs=[smem, smem] + [pl.BlockSpec(memory_space=pl.ANY)] * 5,
        out_specs=(vmem, vmem),
        scratch_shapes=[
            pltpu.VMEM((cells, line_length), f32),
            pltpu.VMEM((cells, line_length), jnp.int32),
            pltpu.VMEM((cells, line_length), jnp.int32),
            pltpu.VMEM((cells, line_length), f32),
            pltpu.VMEM((cells, line_length), f32),
            pltpu.VMEM((cols, cells, width), f32),
            pltpu.VMEM((cols, cells, width), f32),
            pltpu.VMEM((ITERS + 1, cols, cells + 16, width), f32),
            pltpu.VMEM((cols, cells, width), f32),
            pltpu.VMEM((x_blocks, cells, cells), f32),
            pltpu.VMEM((cells, cells), f32),
            pltpu.VMEM((x_blocks, cells, cells), jnp.bfloat16),
            pltpu.VMEM((x_blocks, cells, cells), jnp.bfloat16),
            pltpu.VMEM((cells, cells), jnp.bfloat16),
            pltpu.VMEM((cells, cells), jnp.bfloat16),
            pltpu.VMEM((cols, cells, 128), f32),
            pltpu.VMEM((8, width), f32),
            pltpu.VMEM((8, 128), f32),
            pltpu.VMEM((8, 128), f32),
            pltpu.VMEM((ITERS, 8, lines), f32),
            pltpu.VMEM((ITERS, 8 * cols, lines), f32),
            pltpu.VMEM((ITERS, 8, lines), f32),
            pltpu.VMEM((ITERS, 16, lines), f32),
            pltpu.VMEM((ITERS, 2 * cols, width), f32),
            pltpu.VMEM((ITERS, 2 * cols * rows, width), f32),
            pltpu.VMEM((8, 128), f32),
            pltpu.VMEM((cols - 1, 8, 128), f32),
            pltpu.VMEM((8, 128), f32),
            pltpu.VMEM((rows - 1, 8, 128), f32),
            dma((x_blocks + 5,)),
            dma((4, cols - 1)),
            dma((4, cols - 1)),
            dma((cols - 1,)),
            dma((cols - 1,)),
            dma((ITERS, cols - 1)),
            dma((ITERS, cols - 1)),
            dma((ITERS, 2)),
            dma((ITERS, 2)),
            dma((ITERS, 2)),
            dma((ITERS, 2)),
            dma((ITERS, rows - 1)),
            dma((ITERS, rows - 1)),
            dma((cols - 1,)),
            dma((cols - 1,)),
            dma((rows - 1,)),
            dma((rows - 1,)),
        ],
        compiler_params=pltpu.CompilerParams(
            has_side_effects=True, vmem_limit_bytes=60 * 1024 * 1024
        ),
        name="line_iterations",
    )(
        corners,
        z_inverse,
        energy[0],
        damage_old[0],
        crack_seeds[0],
        irreversible[0],
        line_inverses,
    )
    return damage[None], norms[:ITERS, 0]


def solution(mesh):
    def local_any(energy, damage_old, crack_seeds, irreversible, line_inverses, z_inverse):
        rows, cols = mesh.shape["row"], mesh.shape["col"]
        block_cells = line_inverses.shape[1]
        width = energy.shape[2] // cols
        whole_blocks = (
            energy.shape[0] == 1
            and energy.shape[1] == block_cells
            and width % block_cells == 0
            and 2 * (width // block_cells) <= 8
            and 2 * cols == 8
            and 8 * max(rows, cols) <= 128
            and min(rows, cols) > 2
        )
        chosen = local if whole_blocks else local_turned
        return chosen(energy, damage_old, crack_seeds, irreversible, line_inverses, z_inverse)

    return jax.shard_map(
        local_any,
        mesh=mesh,
        in_specs=(
            P("col", "row", None),
            P("col", "row", None),
            P("col", "row", None),
            P("col", "row", None),
            P(),
            P(),
        ),
        out_specs=(P("col", "row", None), P()),
        check_vma=False,
    )
```

```python
import functools

import jax
import jax.numpy as jnp
from jax import lax
from jax.experimental import pallas as pl
from jax.experimental.pallas import tpu as pltpu
from jax.sharding import PartitionSpec as P

ITERS = 2


KAPPA = 2.0
STEP = 0.02
COUPLE = 0.5
EPSILON = 1e-06
HIGHEST = lax.Precision.HIGHEST


def second_difference(grid_field, along):
    extent = grid_field.shape[along]
    forward_diff = lax.slice_in_dim(grid_field, 1, extent, axis=along) - lax.slice_in_dim(
        grid_field, 0, extent - 1, axis=along
    )
    zero_shape = list(grid_field.shape)
    zero_shape[along] = 1
    zero_rim = jnp.zeros(zero_shape, grid_field.dtype)
    ahead = jnp.concatenate([forward_diff, zero_rim], axis=along)
    behind = jnp.concatenate([zero_rim, forward_diff], axis=along)
    return ahead - behind


def line_solve(line_rows, inverses):
    block_count, block_cells, _ = inverses.shape
    line_count = line_rows.shape[0]
    blocks = line_rows.reshape(line_count, block_count, block_cells)
    products = jnp.einsum("rkb,kcb->rkc", blocks, inverses, precision=lax.Precision.HIGHEST)
    first_col = inverses[:, :, 0]
    last_col = inverses[:, :, block_cells - 1]
    incoming = [jnp.zeros((line_count,), line_rows.dtype)]
    for block_index in range(block_count - 1):
        incoming.append(
            products[:, block_index, block_cells - 1]
            + COUPLE * incoming[block_index] * inverses[block_index, block_cells - 1, 0]
        )
    inflow = jnp.stack(incoming, axis=1)
    forward = products + COUPLE * inflow[:, :, None] * first_col[None]
    head_terms = [jnp.zeros((line_count,), line_rows.dtype) for block_index in range(block_count)]
    carried = forward[:, block_count - 1, 0]
    for block_index in range(block_count - 2, -1, -1):
        head_terms[block_index] = carried
        carried = (
            forward[:, block_index, 0]
            + COUPLE * carried * inverses[block_index, 0, block_cells - 1]
        )
    outflow = jnp.stack(head_terms, axis=1)
    solved = forward + COUPLE * outflow[:, :, None] * last_col[None]
    return solved.reshape(line_count, block_count * block_cells)


def local_turned(energy, damage_old, crack_seeds, irreversible, line_inverses, z_inverse):
    planes, rows_here, line_length = energy.shape
    row_count = lax.axis_size("row")
    col_count = lax.axis_size("col")
    total_planes = planes * col_count
    cell_count = total_planes * rows_here * row_count * line_length
    seeded = crack_seeds == 1
    damage = jnp.where(seeded, 1.0, damage_old)
    lower_bound = jnp.where(irreversible == 1, damage_old, 0.0)
    own_sums = []
    for sweep_index in range(ITERS):
        local_lap = second_difference(damage, 2)
        partial_value = energy - (1.0 + energy) * damage + KAPPA * local_lap
        moved_part, moved_damage = (
            lax.all_to_all(
                lax.all_to_all(
                    jnp.swapaxes(partial_value, 1, 2),
                    "row",
                    split_axis=1,
                    concat_axis=2,
                    tiled=True,
                ),
                "col",
                split_axis=1,
                concat_axis=0,
                tiled=True,
            ),
            lax.all_to_all(
                lax.all_to_all(
                    jnp.swapaxes(damage, 1, 2), "row", split_axis=1, concat_axis=2, tiled=True
                ),
                "col",
                split_axis=1,
                concat_axis=0,
                tiled=True,
            ),
        )
        lap_rest = second_difference(moved_damage, 2) + second_difference(moved_damage, 0)
        turned = moved_part + KAPPA * lap_rest
        turned_shape = turned.shape
        along_y = line_solve(turned.reshape(-1, turned_shape[2]), line_inverses).reshape(
            turned_shape
        )
        along_z = jnp.einsum("zk,kxy->zxy", z_inverse, along_y, precision=lax.Precision.HIGHEST)
        gathered = lax.all_to_all(
            lax.all_to_all(along_z, "row", split_axis=2, concat_axis=1, tiled=True),
            "col",
            split_axis=0,
            concat_axis=1,
            tiled=True,
        )
        piece_cells = gathered.shape[1] // (row_count * col_count)
        reordered = gathered.reshape(planes, col_count, row_count, piece_cells, rows_here)
        restored = jnp.transpose(reordered, (0, 4, 2, 1, 3)).reshape(planes, rows_here, line_length)
        update = STEP * line_solve(restored.reshape(-1, line_length), line_inverses).reshape(
            restored.shape
        )
        clamped = jnp.minimum(jnp.maximum(damage + update, lower_bound), 1.0)
        renewed = jnp.where(seeded, 1.0, clamped)
        own_sum = jnp.sum((renewed - damage) ** 2)
        own_sums.append(own_sum)
        damage = renewed
    global_sums = lax.psum(jnp.stack(own_sums), ("row", "col"))
    update_norms = jnp.sqrt(global_sums / cell_count + EPSILON) / STEP
    return (damage, update_norms)


def line_kernel(
    shape,
    corners,
    z_inv,
    energy,
    damage_hbm,
    seeds_hbm,
    irreversible_hbm,
    inverses,
    out,
    norms,
    damage_old,
    crack_seeds,
    irreversible,
    start,
    bound,
    ez,
    fz,
    dz,
    mix,
    gx,
    gy,
    gx_high,
    gx_low,
    gy_high,
    gy_low,
    h_in,
    gend,
    ab_x,
    ab_y,
    x_send,
    x_all,
    h_send,
    h_recv,
    y_send,
    y_all,
    s_send,
    s_col,
    s_row_send,
    s_row,
    local_sems,
    move_send,
    move_recv,
    back_send,
    back_recv,
    x_ssem,
    x_rsem,
    h_ssem,
    h_rsem,
    v_ssem,
    v_rsem,
    y_ssem,
    y_rsem,
    sc_ssem,
    sc_rsem,
    sr_ssem,
    sr_rsem,
):
    rows, cols, cells, width, x_blocks, blocks, cell_count = shape
    planes = cols
    last = cells - 1
    row, col = lax.axis_index("row"), lax.axis_index("col")
    ends = 8
    tail = 8 - x_blocks

    def slab(who):
        return pl.ds(pl.multiple_of(who * width, width), width)

    def send(src, dst, ssem, rsem, **where):
        copy = pltpu.make_async_remote_copy(
            src_ref=src, dst_ref=dst, send_sem=ssem, recv_sem=rsem,
            device_id=where, device_id_type=pl.DeviceIdType.MESH,
        )
        copy.start()
        return copy

    def weighted(weights, field, kept):
        total = None
        for n in kept:
            term = weights[:, n : n + 1] * field[n : n + 1]
            total = term if total is None else total + term
        return total

    def split(a):
        high = a.astype(jnp.bfloat16)
        return high, (a - high.astype(jnp.float32)).astype(jnp.bfloat16)

    def dot3(a, b):
        def part(u, v):
            return jnp.dot(u, v, preferred_element_type=jnp.float32)

        return part(a[0], b[0]) + (part(a[0], b[1]) + part(a[1], b[0]))

    def line_ends(field):
        tile_lane = lax.broadcasted_iota(jnp.int32, (cells, 128), 1)
        packed = field[:, :128]
        for j in range(x_blocks):
            head = field[:, j * cells : j * cells + 128]
            end = field[:, (j + 1) * cells - 128 : (j + 1) * cells]
            if j > 0:
                head = pltpu.roll(head, j, 1)
                end = pltpu.roll(end, 128 - j, 1)
            packed = jnp.where(tile_lane == j, head, packed)
            packed = jnp.where(tile_lane == 127 - j, end, packed)
        turned = packed.T
        at = lax.broadcasted_iota(jnp.int32, (8, cells), 0)
        kept = (at < x_blocks) | (at >= 8 - x_blocks)
        return jnp.where(kept, jnp.where(at < x_blocks, turned[:8], turned[120:]), 0.0)

    fetch = [
        pltpu.make_async_copy(inverses.at[col * x_blocks + j], gx.at[j], local_sems.at[j])
        for j in range(x_blocks)
    ]
    fetch.append(pltpu.make_async_copy(inverses.at[row], gy, local_sems.at[x_blocks]))
    pulls = [
        pltpu.make_async_copy(damage_hbm, damage_old, local_sems.at[x_blocks + 1]),
        pltpu.make_async_copy(seeds_hbm, crack_seeds, local_sems.at[x_blocks + 2]),
        pltpu.make_async_copy(irreversible_hbm, irreversible, local_sems.at[x_blocks + 3]),
        pltpu.make_async_copy(energy.at[:, slab(col)], ez.at[col], local_sems.at[x_blocks + 4]),
    ]

    moves = []
    inside = pl.ds(8, cells)

    def move(index, src, landing, part=slice(None)):
        sent = []
        for o in range(1, cols):
            peer = lax.rem(col + o, cols)
            sent.append(
                send(src.at[part, slab(peer)], landing, move_send.at[index, o - 1],
                     move_recv.at[index, o - 1], col=peer)
            )
        moves.append(sent)

    move(0, energy, ez.at[col])
    for copy in pulls + fetch:
        copy.start()
    for copy in pulls:
        copy.wait()

    @pl.loop(0, cells // 16)
    def _(i):
        at = pl.ds(pl.multiple_of(i * 16, 16), 16)
        old = damage_old[at, :]
        seeded = crack_seeds[at, :] == 1
        start[at, :] = jnp.where(seeded, 1.0, old)
        bound[at, :] = jnp.where(seeded, 1.0, jnp.where(irreversible[at, :] == 1, old, 0.0))

    move(1, start, dz.at[0, col, inside, :])
    dz[0, col, inside, :] = start[:, slab(col)]
    fz[col] = bound[:, slab(col)]

    lane = lax.broadcasted_iota(jnp.int32, (8, 128), 1)
    sub = lax.broadcasted_iota(jnp.int32, (8, 128), 0)

    def carries(first, final, own):
        zero = jnp.zeros((8, 128), jnp.float32)
        incoming = [zero]
        for k in range(blocks - 1):
            at_last = jnp.where(lane == final(k), 1.0, 0.0)
            incoming.append(at_last + COUPLE * corners[1, k] * incoming[k])
        head = [
            jnp.where(lane == first(k), 1.0, 0.0) + COUPLE * corners[0, k] * incoming[k]
            for k in range(blocks)
        ]
        carried = head[blocks - 1]
        outgoing = [zero] * blocks
        for k in range(blocks - 2, -1, -1):
            outgoing[k] = carried
            carried = head[k] + COUPLE * corners[2, k] * carried
        picked = zero
        even = lax.rem(sub, 2) == 0
        for k in range(blocks):
            value = jnp.where(even, incoming[k], outgoing[k])
            picked = picked + jnp.where(own == k, COUPLE * value, 0.0)
        return picked

    half = lax.div(sub, 2)
    ab_x[...] = carries(
        lambda k: ends * (k // x_blocks) + k % x_blocks,
        lambda k: ends * (k // x_blocks) + 7 - k % x_blocks,
        jnp.where(half < x_blocks, col * x_blocks + half, -1),
    )
    ab_y[...] = carries(
        lambda k: 2 * planes * k + 2 * half,
        lambda k: 2 * planes * k + 2 * half + 1,
        row + 0 * sub,
    )

    for copy in fetch:
        copy.wait()
    gend[...] = jnp.zeros_like(gend)
    for j in range(x_blocks):
        turned = gx[j].T
        gx_high[j], gx_low[j] = split(turned)
        block = slice(j * cells, (j + 1) * cells)
        gend[2 * j : 2 * j + 1, block] = turned[:1]
        gend[2 * j + 1 : 2 * j + 2, block] = turned[last:]
    gy_high[...], gy_low[...] = split(gy[...])

    wide_row = lax.broadcasted_iota(jnp.int32, (8, width), 0)
    wide_lane = lax.broadcasted_iota(jnp.int32, (8, width), 1)
    has_left, has_right = col > 0, col < cols - 1
    degree_x = (
        2.0
        - jnp.where((wide_lane == 0) & jnp.logical_not(has_left), 1.0, 0.0)
        - jnp.where((wide_lane == width - 1) & jnp.logical_not(has_right), 1.0, 0.0)
    )
    at_first, at_last = wide_lane == 0, wide_lane == width - 1
    upper = jnp.where(row > 0, 1.0, 0.0)
    lower = jnp.where(row < rows - 1, 1.0, 0.0)

    def finish(sent):
        for copy in sent:
            copy.wait()

    def line_rows(z):
        return pl.ds(pl.multiple_of(z * cells, cells), cells)

    finish(moves[1])

    totals = []
    for it in range(ITERS):
        @pl.loop(0, planes)
        def _(z):
            h_send[it, :, line_rows(z)] = line_ends(dz[it, z, inside, :])

        halo = [
            send(h_send.at[it], h_recv.at[it, pl.ds(0, 8), :], h_ssem.at[it, 0], h_rsem.at[it, 0],
                 col=lax.rem(col + 1, cols)),
            send(h_send.at[it], h_recv.at[it, pl.ds(8, 8), :], h_ssem.at[it, 1], h_rsem.at[it, 1],
                 col=lax.rem(col + cols - 1, cols)),
            send(dz.at[it, :, pl.ds(cells, 8), :], dz.at[it, :, pl.ds(0, 8), :], v_ssem.at[it, 0],
                 v_rsem.at[it, 0], row=lax.rem(row + 1, rows)),
            send(dz.at[it, :, pl.ds(8, 8), :], dz.at[it, :, pl.ds(cells + 8, 8), :],
                 v_ssem.at[it, 1], v_rsem.at[it, 1], row=lax.rem(row + rows - 1, rows)),
        ]
        if it == 0:
            finish(moves[0])
            pieces = [slice(0, cells // 2), slice(cells // 2, cells)]
            move(2, bound, fz.at[col, pieces[0], :], pieces[0])
        finish(halo)

        @pl.loop(0, planes)
        def _(z):
            left = h_recv[it, tail : tail + 1, line_rows(z)]
            right = h_recv[it, 8:9, line_rows(z)]
            at = lax.broadcasted_iota(jnp.int32, (128, cells), 0)
            left = jnp.where((at == 0) & has_left, left, 0.0)
            right = jnp.where((at == 127) & has_right, right, 0.0)
            h_in[z] = (left + right).T

        @pl.loop(0, cells // 8)
        def _(i):
            near = pl.ds(pl.multiple_of(i * 8, 8), 24)
            here = pl.ds(pl.multiple_of(i * 8, 8), 8)
            y_at = wide_row + i * 8
            top = jnp.where(y_at == 0, upper, 1.0)
            bottom = jnp.where(y_at == last, lower, 1.0)
            wins = [dz[it, z, near, :] for z in range(planes)]
            mids = [w[8:16] for w in wins]
            residual = []
            for z in range(planes):
                d = mids[z]
                above = pltpu.roll(wins[z], 1, 0)[8:16]
                below = pltpu.roll(wins[z], 23, 0)[8:16]
                lap = top * (above - d) + bottom * (below - d)
                lap = lap + jnp.where(at_first, 0.0, pltpu.roll(d, 1, 1))
                lap = lap + jnp.where(at_last, 0.0, pltpu.roll(d, width - 1, 1))
                edges = h_in[z, here, :]
                lap = lap + jnp.where(at_first, jnp.tile(edges, (1, width // 128)), 0.0)
                lap = lap + jnp.where(at_last, jnp.tile(edges, (1, width // 128)), 0.0)
                lap = lap - degree_x * d
                if z > 0:
                    lap = lap + (mids[z - 1] - d)
                if z < planes - 1:
                    lap = lap + (mids[z + 1] - d)
                e = ez[z, here, :]
                residual.append(e - (1.0 + e) * d + KAPPA * lap)
            for z in range(planes):
                total = z_inv[z, 0] * residual[0]
                for k in range(1, planes):
                    total = total + z_inv[z, k] * residual[k]
                mix[z, here, :] = total

        @pl.loop(0, planes)
        def _(z):
            along = jnp.concatenate(
                [
                    dot3(
                        split(mix[z, :, j * cells : (j + 1) * cells]), (gx_high[j], gx_low[j])
                    )
                    for j in range(x_blocks)
                ],
                axis=1,
            )
            both = dot3((gy_high[...], gy_low[...]), split(along))
            mix[z] = both
            x_send[it, :, line_rows(z)] = line_ends(both)

        swaps = []
        for o in range(1, cols):
            swaps.append(
                send(x_send.at[it], x_all.at[it, pl.ds(pl.multiple_of(col * 8, 8), 8), :],
                     x_ssem.at[it, o - 1], x_rsem.at[it, o - 1], col=lax.rem(col + o, cols))
            )
        x_all[it, pl.ds(pl.multiple_of(col * 8, 8), 8), :] = x_send[it]
        if it == 0:
            move(3, bound, fz.at[col, pieces[1], :], pieces[1])
        finish(swaps)

        for z in range(planes):
            kept = [
                ends * c + n for c in range(cols) for n in range(ends)
                if n < x_blocks or n >= ends - x_blocks
            ]
            carry = weighted(ab_x[...], x_all[it, :, z * cells : (z + 1) * cells], kept)
            carry = jnp.concatenate([carry, jnp.zeros((120, cells), jnp.float32)], axis=0).T
            parts = []
            for j in range(x_blocks):
                block = slice(j * cells, (j + 1) * cells)
                enter = carry[:, 2 * j : 2 * j + 1] * gend[2 * j : 2 * j + 1, block]
                leave = carry[:, 2 * j + 1 : 2 * j + 2] * gend[2 * j + 1 : 2 * j + 2, block]
                parts.append(mix[z, :, block] + enter + leave)
            value = jnp.concatenate(parts, axis=1)
            mix[z] = value
            y_send[it, 2 * z : 2 * z + 1, :] = value[:1]
            y_send[it, 2 * z + 1 : 2 * z + 2, :] = value[last:]

        swaps = []
        own = pl.ds(pl.multiple_of(row * 2 * planes, 2 * planes), 2 * planes)
        for o in range(1, rows):
            swaps.append(
                send(y_send.at[it], y_all.at[it, own, :], y_ssem.at[it, o - 1],
                     y_rsem.at[it, o - 1], row=lax.rem(row + o, rows))
            )
        y_all[it, own, :] = y_send[it]
        finish(swaps)
        if it == 0:
            finish(moves[2] + moves[3])
        carry_y = weighted(ab_y[...], y_all[it], range(rows * 2 * planes))

        squares = jnp.zeros((8, width), jnp.float32)
        for z in range(planes):
            enter, leave = carry_y[2 * z : 2 * z + 1], carry_y[2 * z + 1 : 2 * z + 2]

            def settle(i, acc, z=z, enter=enter, leave=leave):
                here = pl.ds(pl.multiple_of(i * 8, 8), 8)
                padded = pl.ds(pl.multiple_of(i * 8 + 8, 8), 8)
                g_first, g_last = gy[here, 0:1], gy[here, last : last + 1]
                solved = mix[z, here, :] + g_first * enter + g_last * leave
                d = dz[it, z, padded, :]
                renewed = jnp.minimum(jnp.maximum(d + STEP * solved, fz[z, here, :]), 1.0)
                dz[it + 1, z, padded, :] = renewed
                change = renewed - d
                return acc + change * change

            squares = lax.fori_loop(0, cells // 8, settle, squares, unroll=2)
        totals.append(jnp.sum(squares))

    s_send[...] = jnp.where(sub == 0, totals[0], jnp.where(sub == 1, totals[1], 0.0))
    final = dz.at[ITERS]
    shares = []
    for o in range(1, cols):
        shares.append(
            send(s_send, s_col.at[o - 1], sc_ssem.at[o - 1], sc_rsem.at[o - 1],
                 col=lax.rem(col + o, cols))
        )
    backs = []
    for o in range(1, cols):
        peer = lax.rem(col + o, cols)
        backs.append(
            send(final.at[peer, inside, :], out.at[:, slab(col)], back_send.at[o - 1],
                 back_recv.at[o - 1], col=peer)
        )
    out[:, slab(col)] = final[col, inside, :]
    finish(shares)
    total = s_send[...]
    for o in range(1, cols):
        total = total + s_col[o - 1]
    s_row_send[...] = total
    shares = []
    for o in range(1, rows):
        shares.append(
            send(s_row_send, s_row.at[o - 1], sr_ssem.at[o - 1], sr_rsem.at[o - 1],
                 row=lax.rem(row + o, rows))
        )
    finish(shares)
    for o in range(1, rows):
        total = total + s_row[o - 1]
    norms[...] = jnp.sqrt(total / cell_count + EPSILON) / STEP
    finish(backs)


def local(energy, damage_old, crack_seeds, irreversible, line_inverses, z_inverse):
    planes, cells, line_length = energy.shape
    rows, cols = lax.axis_size("row"), lax.axis_size("col")
    blocks, _, _ = line_inverses.shape
    width = line_length // cols
    x_blocks = width // cells
    last = cells - 1
    lines = cols * cells
    shape = (rows, cols, cells, width, x_blocks, blocks, float(cols * rows * cells * line_length))
    corners = jnp.stack(
        [line_inverses[:, 0, 0], line_inverses[:, last, 0], line_inverses[:, 0, last]]
    )
    f32 = jnp.float32
    dma = pltpu.SemaphoreType.DMA
    vmem = pl.BlockSpec(memory_space=pltpu.VMEM)
    smem = pl.BlockSpec(memory_space=pltpu.SMEM)
    damage, norms = pl.pallas_call(
        functools.partial(line_kernel, shape),
        out_shape=(
            jax.ShapeDtypeStruct((cells, line_length), f32),
            jax.ShapeDtypeStruct((8, 128), f32),
        ),
        in_specs=[smem, smem] + [pl.BlockSpec(memory_space=pl.ANY)] * 5,
        out_specs=(vmem, vmem),
        scratch_shapes=[
            pltpu.VMEM((cells, line_length), f32),
            pltpu.VMEM((cells, line_length), jnp.int32),
            pltpu.VMEM((cells, line_length), jnp.int32),
            pltpu.VMEM((cells, line_length), f32),
            pltpu.VMEM((cells, line_length), f32),
            pltpu.VMEM((cols, cells, width), f32),
            pltpu.VMEM((cols, cells, width), f32),
            pltpu.VMEM((ITERS + 1, cols, cells + 16, width), f32),
            pltpu.VMEM((cols, cells, width), f32),
            pltpu.VMEM((x_blocks, cells, cells), f32),
            pltpu.VMEM((cells, cells), f32),
            pltpu.VMEM((x_blocks, cells, cells), jnp.bfloat16),
            pltpu.VMEM((x_blocks, cells, cells), jnp.bfloat16),
            pltpu.VMEM((cells, cells), jnp.bfloat16),
            pltpu.VMEM((cells, cells), jnp.bfloat16),
            pltpu.VMEM((cols, cells, 128), f32),
            pltpu.VMEM((8, width), f32),
            pltpu.VMEM((8, 128), f32),
            pltpu.VMEM((8, 128), f32),
            pltpu.VMEM((ITERS, 8, lines), f32),
            pltpu.VMEM((ITERS, 8 * cols, lines), f32),
            pltpu.VMEM((ITERS, 8, lines), f32),
            pltpu.VMEM((ITERS, 16, lines), f32),
            pltpu.VMEM((ITERS, 2 * cols, width), f32),
            pltpu.VMEM((ITERS, 2 * cols * rows, width), f32),
            pltpu.VMEM((8, 128), f32),
            pltpu.VMEM((cols - 1, 8, 128), f32),
            pltpu.VMEM((8, 128), f32),
            pltpu.VMEM((rows - 1, 8, 128), f32),
            dma((x_blocks + 5,)),
            dma((4, cols - 1)),
            dma((4, cols - 1)),
            dma((cols - 1,)),
            dma((cols - 1,)),
            dma((ITERS, cols - 1)),
            dma((ITERS, cols - 1)),
            dma((ITERS, 2)),
            dma((ITERS, 2)),
            dma((ITERS, 2)),
            dma((ITERS, 2)),
            dma((ITERS, rows - 1)),
            dma((ITERS, rows - 1)),
            dma((cols - 1,)),
            dma((cols - 1,)),
            dma((rows - 1,)),
            dma((rows - 1,)),
        ],
        compiler_params=pltpu.CompilerParams(
            has_side_effects=True, vmem_limit_bytes=60 * 1024 * 1024
        ),
        name="line_iterations",
    )(
        corners,
        z_inverse,
        energy[0],
        damage_old[0],
        crack_seeds[0],
        irreversible[0],
        line_inverses,
    )
    return damage[None], norms[:ITERS, 0]


def solution(mesh):
    def local_any(energy, damage_old, crack_seeds, irreversible, line_inverses, z_inverse):
        rows, cols = mesh.shape["row"], mesh.shape["col"]
        block_cells = line_inverses.shape[1]
        width = energy.shape[2] // cols
        whole_blocks = (
            energy.shape[0] == 1
            and energy.shape[1] == block_cells
            and width % block_cells == 0
            and 2 * (width // block_cells) <= 8
            and 2 * cols == 8
            and 8 * max(rows, cols) <= 128
            and min(rows, cols) > 2
        )
        chosen = local if whole_blocks else local_turned
        return chosen(energy, damage_old, crack_seeds, irreversible, line_inverses, z_inverse)

    return jax.shard_map(
        local_any,
        mesh=mesh,
        in_specs=(
            P("col", "row", None),
            P("col", "row", None),
            P("col", "row", None),
            P("col", "row", None),
            P(),
            P(),
        ),
        out_specs=(P("col", "row", None), P()),
        check_vma=False,
    )
```
